8 devices in a mesh: dp: 1 (over z), cx: 2 (over y), cy: 4 (over x, core).
Axes of the slice: x: 2, y: 2, z: 1, core: 2. Of those that a mesh axis runs over, the one named last changes fastest.
Arguments:
- x: bfloat16 [1, 2048, 1536], P('dp', ('cx', 'cy'))
- w_qkv: bfloat16 [1536, 4608], replicated
- w_o: bfloat16 [24, 64, 1536], replicated
Outputs:
- output: bfloat16 [1, 2048, 1536], P('dp', ('cx', 'cy'))
All inputs are finite; a program needn't handle non-finite values.
Results may differ from the reference program's by a relative error of at most 0.00800223.
Values are sent between devices in bfloat16 or wider.
A program may use at most 1 GiB of HBM per device.

```python
import math
import jax
import jax.numpy as jnp
from jax import lax

SEQ_LEN = 2048
NUM_HEADS = 24
HEAD_DIM = 64


def setup_inputs(seed: int = 0, part: int = 0) -> dict:
    model_width = NUM_HEADS * HEAD_DIM
    base_key = jax.random.key(seed)
    token_key = jax.random.fold_in(jax.random.fold_in(base_key, part), 1)
    qkv_key = jax.random.fold_in(base_key, 2)
    out_key = jax.random.fold_in(base_key, 3)
    logit_std = math.sqrt(max(math.log(SEQ_LEN / 20.0), 2.0))
    qk_gain = math.sqrt(logit_std)
    col_gain = jnp.concatenate([jnp.full((2 * model_width,), qk_gain, jnp.float32), jnp.ones((model_width,), jnp.float32)])
    tokens = jax.random.normal(token_key, (1, SEQ_LEN, model_width), jnp.float32)
    w_qkv = jax.random.normal(qkv_key, (model_width, 3 * model_width), jnp.float32) * (model_width ** -0.5) * col_gain
    w_out = jax.random.normal(out_key, (NUM_HEADS, HEAD_DIM, model_width), jnp.float32) * (2.5 * model_width ** -0.5)
    return {"x": tokens.astype(jnp.bfloat16), "w_qkv": w_qkv.astype(jnp.bfloat16), "w_o": w_out.astype(jnp.bfloat16)}


def reference(x, w_qkv, w_o):
    model_width = NUM_HEADS * HEAD_DIM
    q_block = math.gcd(SEQ_LEN, 256)
    n_blocks = SEQ_LEN // q_block
    inv_sqrt = 1.0 / math.sqrt(HEAD_DIM)
    qkv_rows = jnp.dot(x[0], w_qkv, preferred_element_type=jnp.float32).astype(jnp.bfloat16)
    qkv_rows = jnp.transpose(qkv_rows.reshape(SEQ_LEN, 3, NUM_HEADS, HEAD_DIM), (1, 2, 0, 3))

    def head_attend(head_args):
        q_head, k_head, v_head = head_args
        k_full = k_head.astype(jnp.float32)
        v_full = v_head.astype(jnp.float32)
        q_blocks = q_head.astype(jnp.float32).reshape(n_blocks, q_block, HEAD_DIM)

        def block_attend(q_rows):
            logits = jnp.dot(q_rows, k_full.T, preferred_element_type=jnp.float32) * inv_sqrt
            row_max = jnp.max(logits, axis=-1, keepdims=True)
            weights = jnp.exp(logits - row_max)
            row_sum = jnp.sum(weights, axis=-1, keepdims=True)
            return jnp.dot(weights, v_full, preferred_element_type=jnp.float32) / row_sum

        return lax.map(block_attend, q_blocks).reshape(SEQ_LEN, HEAD_DIM)

    attn_rows = lax.map(head_attend, (qkv_rows[0], qkv_rows[1], qkv_rows[2]))
    attn_rows = jnp.transpose(attn_rows, (1, 0, 2)).reshape(SEQ_LEN, model_width).astype(jnp.bfloat16)
    result = jnp.dot(attn_rows, w_o.reshape(model_width, model_width), preferred_element_type=jnp.float32)
    return result.astype(jnp.bfloat16)[None]
```

```python
import math

import jax
import jax.numpy as jnp
from jax import lax
from jax.experimental import pallas as pl
from jax.experimental.pallas import tpu as pltpu
from jax.sharding import PartitionSpec as P

MESH = pl.DeviceIdType.MESH
BF16 = jnp.bfloat16
F32 = jnp.float32
NSUB = 2


def _nt(a, b):
    return lax.dot_general(a, b, (((1,), (1,)), ((), ())), preferred_element_type=F32)


def _tn(a, b):
    return lax.dot_general(a, b, (((0,), (0,)), ((), ())), preferred_element_type=F32)


def _nn(a, b):
    return lax.dot_general(a, b, (((1,), (0,)), ((), ())), preferred_element_type=F32)


def _kernel(dims, x_hbm, wqkv_hbm, wo_hbm, y_ref,
            xs, wq, wk, wv, wvt, wo, ks, vts, qz, ms, ls, acc, osend, omine, orecv,
            wsem, ssem, rsem, osem):
    tok, width, heads, hd = dims
    cols = heads * hd
    half = tok // 2
    sub = half // NSUB
    scale = (hd ** -0.5) * math.log2(math.e)

    dp, cx, cy = lax.axis_index("dp"), lax.axis_index("cx"), lax.axis_index("cy")
    core = lax.rem(cy, 2)
    mate = (dp, cx, cy + 1 - 2 * core)
    xn = (dp, cx, lax.rem(cy + 2, 4))
    yn = (dp, 1 - cx, cy)

    def wcopy(i, src, dst):
        return pltpu.make_async_copy(src, dst, wsem.at[i])

    g0 = pl.multiple_of(core * cols, cols)
    g1 = pl.multiple_of((1 - core) * cols, cols)
    loads = [
        wcopy(0, x_hbm, xs.at[0, pl.ds(0, tok), :]),
        wcopy(1, wqkv_hbm.at[:, pl.ds(g0, cols)], wq),
        wcopy(2, wqkv_hbm.at[:, pl.ds(pl.multiple_of(g0 + width, cols), cols)], wk),
        wcopy(3, wqkv_hbm.at[:, pl.ds(pl.multiple_of(g0 + 2 * width, cols), cols)], wv),
        wcopy(4, wo_hbm.at[pl.ds(g0, cols), :], wo.at[0]),
        wcopy(5, wo_hbm.at[pl.ds(g1, cols), :], wo.at[1]),
    ]
    for ld in loads:
        ld.start()

    barrier = pltpu.get_barrier_semaphore()
    for other in (mate, xn, yn):
        pl.semaphore_signal(barrier, inc=1, device_id=other, device_id_type=MESH)
    pl.semaphore_wait(barrier, 3)

    started = []

    def send(i, stage_from, row_from, stage_to, row_to, rows, dev):
        c = pltpu.make_async_remote_copy(
            src_ref=xs.at[stage_from, pl.ds(row_from, rows), :],
            dst_ref=xs.at[stage_to, pl.ds(row_to, rows), :],
            send_sem=ssem.at[i], recv_sem=rsem.at[i],
            device_id=dev, device_id_type=MESH)
        return c

    copies = {}
    n = 0

    def define(key, *a):
        nonlocal n
        copies[key] = send(n, *a)
        n += 1

    define(("own",), 0, 0, 0, tok, tok, mate)
    for st, hx, hy in ((1, 1, 0), (2, 0, 1)):
        for u in range(NSUB):
            define(("x", st, u), 0, hx * half + u * sub, st, u * sub, sub, xn)
            define(("y", st, u), 0, hy * half + u * sub, st, half + u * sub, sub, yn)
            define(("fx", st, u), st, u * sub, st, tok + u * sub, sub, mate)
            define(("fy", st, u), st, half + u * sub, st, tok + half + u * sub, sub, mate)
    for u in range(NSUB):
        define(("x", 3, u), 1, half + u * sub, 3, u * sub, sub, xn)
        define(("y", 3, u), 1, u * sub, 3, half + u * sub, sub, yn)
        define(("fx", 3, u), 3, u * sub, 3, tok + u * sub, sub, mate)
        define(("fy", 3, u), 3, half + u * sub, 3, tok + half + u * sub, sub, mate)

    def start(key):
        copies[key].start()
        started.append(key)

    loads[0].wait()
    start(("own",))
    for st in (1, 2):
        for u in range(NSUB):
            start(("x", st, u))
            start(("y", st, u))

    def project(st, r0):
        rows = xs[st, pl.ds(r0, tok), :]
        ks[pl.ds(r0, tok), :] = _nn(rows, wk[...]).astype(BF16)
        vts[:, pl.ds(r0, tok)] = _nt(wvt[...], rows).astype(BF16)

    def project_q(r0):
        rows = xs[0, pl.ds(r0, tok), :]
        qt = _nn(rows, wq[...]).T.astype(BF16)
        for h in range(heads):
            e = (h % 2) * hd
            qz[h, pl.ds(e, hd), pl.ds(r0, tok)] = qt[h * hd:(h + 1) * hd, :]

    def attend(st):
        def pair(j, carry):
            kp = ks[:, pl.ds(pl.multiple_of(j * 2 * hd, 2 * hd), 2 * hd)]
            for e in range(2):
                h = 2 * j + e
                s = _nn(kp, qz[h])
                mc = jnp.max(s, axis=0, keepdims=True)
                vt = vts[pl.ds(pl.multiple_of(h * hd, hd), hd), :]
                if st == 0:
                    m = mc
                else:
                    m = jnp.maximum(ms[h], mc)
                    alpha = jnp.exp2((ms[h] - m) * scale)
                p = jnp.exp2((s - m) * scale)
                lc = jnp.sum(p, axis=0, keepdims=True)
                o = _nn(vt, p.astype(BF16))
                if st == 0:
                    ls[h] = lc
                    acc[h] = o
                else:
                    ls[h] = ls[h] * alpha + lc
                    acc[h] = acc[h] * alpha + o
                ms[h] = m
            return carry

        lax.fori_loop(0, heads // 2, pair, 0)

    for h in range(heads):
        e = ((h + 1) % 2) * hd
        qz[h, pl.ds(e, hd), :] = jnp.zeros((hd, 2 * tok), BF16)
    loads[1].wait()
    project_q(0)
    loads[2].wait()
    loads[3].wait()
    wvt[...] = wv[...].T
    project(0, 0)
    copies[("own",)].wait_recv()
    project_q(tok)
    project(0, tok)
    attend(0)
    for st in (1, 2, 3):
        for u in range(NSUB):
            copies[("x", st, u)].wait_recv()
            start(("fx", st, u))
            if st == 1:
                start(("y", 3, u))
            copies[("y", st, u)].wait_recv()
            start(("fy", st, u))
            if st == 1:
                start(("x", 3, u))
        project(st, 0)
        for u in range(NSUB):
            copies[("fx", st, u)].wait_recv()
            copies[("fy", st, u)].wait_recv()
        project(st, tok)
        attend(st)

    for h in range(heads):
        o = (acc[h] / ls[h]).T.astype(BF16)
        omine[:, pl.ds(h * hd, hd)] = o[:tok]
        osend[:, pl.ds(h * hd, hd)] = o[tok:]
    oc = pltpu.make_async_remote_copy(
        src_ref=osend, dst_ref=orecv, send_sem=osem.at[0], recv_sem=osem.at[1],
        device_id=mate, device_id_type=MESH)
    oc.start()
    loads[4].wait()
    loads[5].wait()
    y = _nn(omine[...], wo[0])
    oc.wait_recv()
    y_ref[...] = (y + _nn(orecv[...], wo[1])).astype(BF16)
    oc.wait_send()
    for key in started:
        copies[key].wait_send()


def solution(mesh):
    def body(x, w_qkv, w_o):
        tok, width = x.shape[1], x.shape[2]
        heads_all, hd = w_o.shape[0], w_o.shape[1]
        heads = heads_all // 2
        cols = heads * hd
        ncopy = 1 + 3 * 4 * NSUB
        y = pl.pallas_call(
            lambda *r: _kernel((tok, width, heads, hd), *r),
            out_shape=jax.ShapeDtypeStruct((tok, width), BF16),
            in_specs=[pl.BlockSpec(memory_space=pl.ANY)] * 3,
            out_specs=pl.BlockSpec(memory_space=pltpu.VMEM),
            scratch_shapes=[
                pltpu.VMEM((4, 2 * tok, width), BF16),
                pltpu.VMEM((width, cols), BF16),
                pltpu.VMEM((width, cols), BF16),
                pltpu.VMEM((width, cols), BF16),
                pltpu.VMEM((cols, width), BF16),
                pltpu.VMEM((2, cols, width), BF16),
                pltpu.VMEM((2 * tok, cols), BF16),
                pltpu.VMEM((cols, 2 * tok), BF16),
                pltpu.VMEM((heads, 2 * hd, 2 * tok), BF16),
                pltpu.VMEM((heads, 1, 2 * tok), F32),
                pltpu.VMEM((heads, 1, 2 * tok), F32),
                pltpu.VMEM((heads, hd, 2 * tok), F32),
                pltpu.VMEM((tok, cols), BF16),
                pltpu.VMEM((tok, cols), BF16),
                pltpu.VMEM((tok, cols), BF16),
                pltpu.SemaphoreType.DMA((6,)),
                pltpu.SemaphoreType.DMA((ncopy,)),
                pltpu.SemaphoreType.DMA((ncopy,)),
                pltpu.SemaphoreType.DMA((2,)),
            ],
            compiler_params=pltpu.CompilerParams(
                collective_id=0, has_side_effects=True, vmem_limit_bytes=60 * 1024 * 1024),
            name="dit_attention",
        )(x[0], w_qkv, w_o.reshape(heads_all * hd, width))
        return y[None]

    return jax.shard_map(
        body, mesh=mesh,
        in_specs=(P("dp", ("cx", "cy"), None), P(None, None), P(None, None, None)),
        out_specs=P("dp", ("cx", "cy"), None), check_vma=False)
```

```python
import math

import jax
import jax.numpy as jnp
from jax import lax
from jax.experimental import pallas as pl
from jax.experimental.pallas import tpu as pltpu
from jax.sharding import PartitionSpec as P

MESH = pl.DeviceIdType.MESH
BF16 = jnp.bfloat16
F32 = jnp.float32
NSUB = 2


def _nt(a, b):
    return lax.dot_general(a, b, (((1,), (1,)), ((), ())), preferred_element_type=F32)


def _tn(a, b):
    return lax.dot_general(a, b, (((0,), (0,)), ((), ())), preferred_element_type=F32)


def _nn(a, b):
    return lax.dot_general(a, b, (((1,), (0,)), ((), ())), preferred_element_type=F32)


def _kernel(dims, x_hbm, wqkv_hbm, wo_hbm, y_ref,
            xs, wq, wk, wv, wvt, wo, ks, vts, qz, ms, ls, acc, osend, omine, orecv,
            sb0, sb1, mb0, mb1,
            wsem, ssem, rsem, osem):
    tok, width, heads, hd = dims
    cols = heads * hd
    half = tok // 2
    sub = half // NSUB
    scale = (hd ** -0.5) * math.log2(math.e)

    dp, cx, cy = lax.axis_index("dp"), lax.axis_index("cx"), lax.axis_index("cy")
    core = lax.rem(cy, 2)
    mate = (dp, cx, cy + 1 - 2 * core)
    xn = (dp, cx, lax.rem(cy + 2, 4))
    yn = (dp, 1 - cx, cy)

    def wcopy(i, src, dst):
        return pltpu.make_async_copy(src, dst, wsem.at[i])

    g0 = pl.multiple_of(core * cols, cols)
    g1 = pl.multiple_of((1 - core) * cols, cols)
    loads = [
        wcopy(0, x_hbm, xs.at[0, pl.ds(0, tok), :]),
        wcopy(1, wqkv_hbm.at[:, pl.ds(g0, cols)], wq),
        wcopy(2, wqkv_hbm.at[:, pl.ds(pl.multiple_of(g0 + width, cols), cols)], wk),
        wcopy(3, wqkv_hbm.at[:, pl.ds(pl.multiple_of(g0 + 2 * width, cols), cols)], wv),
        wcopy(4, wo_hbm.at[pl.ds(g0, cols), :], wo.at[0]),
        wcopy(5, wo_hbm.at[pl.ds(g1, cols), :], wo.at[1]),
    ]
    for ld in loads:
        ld.start()

    barrier = pltpu.get_barrier_semaphore()
    for other in (mate, xn, yn):
        pl.semaphore_signal(barrier, inc=1, device_id=other, device_id_type=MESH)
    pl.semaphore_wait(barrier, 3)

    started = []

    def send(i, stage_from, row_from, stage_to, row_to, rows, dev):
        c = pltpu.make_async_remote_copy(
            src_ref=xs.at[stage_from, pl.ds(row_from, rows), :],
            dst_ref=xs.at[stage_to, pl.ds(row_to, rows), :],
            send_sem=ssem.at[i], recv_sem=rsem.at[i],
            device_id=dev, device_id_type=MESH)
        return c

    copies = {}
    n = 0

    def define(key, *a):
        nonlocal n
        copies[key] = send(n, *a)
        n += 1

    define(("own",), 0, 0, 0, tok, tok, mate)
    for st, hx, hy in ((1, 1, 0), (2, 0, 1)):
        for u in range(NSUB):
            define(("x", st, u), 0, hx * half + u * sub, st, u * sub, sub, xn)
            define(("y", st, u), 0, hy * half + u * sub, st, half + u * sub, sub, yn)
            define(("fx", st, u), st, u * sub, st, tok + u * sub, sub, mate)
            define(("fy", st, u), st, half + u * sub, st, tok + half + u * sub, sub, mate)
    for u in range(NSUB):
        define(("x", 3, u), 1, half + u * sub, 3, u * sub, sub, xn)
        define(("y", 3, u), 1, u * sub, 3, half + u * sub, sub, yn)
        define(("fx", 3, u), 3, u * sub, 3, tok + u * sub, sub, mate)
        define(("fy", 3, u), 3, half + u * sub, 3, tok + half + u * sub, sub, mate)

    def start(key):
        copies[key].start()
        started.append(key)

    loads[0].wait()
    start(("own",))
    for st in (1, 2):
        for u in range(NSUB):
            start(("x", st, u))
            start(("y", st, u))

    def project(st, r0):
        rows = xs[st, pl.ds(r0, tok), :]
        ks[pl.ds(r0, tok), :] = _nn(rows, wk[...]).astype(BF16)
        vts[:, pl.ds(r0, tok)] = _nt(wvt[...], rows).astype(BF16)

    def project_q(r0):
        rows = xs[0, pl.ds(r0, tok), :]
        qt = _nn(rows, wq[...]).T.astype(BF16)
        for h in range(heads):
            e = (h % 2) * hd
            qz[h, pl.ds(e, hd), pl.ds(r0, tok)] = qt[h * hd:(h + 1) * hd, :]

    def scores(h, pair, rows, r0, sb, mb):
        kp = ks[pl.ds(r0, rows), pl.ds(pl.multiple_of(pair * 2 * hd, 2 * hd), 2 * hd)]
        s = _nn(kp, qz[h])
        sb[pl.ds(0, rows), :] = s
        mb[...] = jnp.max(s, axis=0, keepdims=True)

    def fold(h, rows, r0, sb, mb, first):
        m = mb[...]
        if not first:
            m = jnp.maximum(ms[h], m)
            alpha = jnp.exp2((ms[h] - m) * scale)
        p = jnp.exp2((sb[pl.ds(0, rows), :] - m) * scale)
        l = jnp.sum(p, axis=0, keepdims=True)
        o = _nn(vts[pl.ds(pl.multiple_of(h * hd, hd), hd), pl.ds(r0, rows)], p.astype(BF16))
        if not first:
            l = ls[h] * alpha + l
            o = acc[h] * alpha + o
        return m, l, o

    def keep(h, mlo):
        ms[h], ls[h], acc[h] = mlo

    def attend(rows, r0, first=False, last=False):
        scores(0, 0, rows, r0, sb0, mb0)

        def pair(j, carry):
            nxt = jnp.minimum(j + 1, heads // 2 - 1)
            scores(2 * j + 1, j, rows, r0, sb1, mb1)
            even = fold(2 * j, rows, r0, sb0, mb0, first)
            if not last:
                keep(2 * j, even)
            scores(2 * nxt, nxt, rows, r0, sb0, mb0)
            odd = fold(2 * j + 1, rows, r0, sb1, mb1, first)
            if not last:
                keep(2 * j + 1, odd)
            else:
                o = jnp.concatenate([even[2] / even[1], odd[2] / odd[1]], axis=0).T.astype(BF16)
                at = pl.ds(pl.multiple_of(j * 2 * hd, 2 * hd), 2 * hd)
                omine[:, at] = o[:tok]
                osend[:, at] = o[tok:]
            return carry

        lax.fori_loop(0, heads // 2, pair, 0)

    for h in range(heads):
        e = ((h + 1) % 2) * hd
        qz[h, pl.ds(e, hd), :] = jnp.zeros((hd, 2 * tok), BF16)
    loads[1].wait()
    project_q(0)
    loads[2].wait()
    loads[3].wait()
    wvt[...] = wv[...].T
    project(0, 0)
    copies[("own",)].wait_recv()
    project_q(tok)
    project(0, tok)
    attend(2 * tok, 0, first=True)
    for st in (1, 2, 3):
        for u in range(NSUB):
            copies[("x", st, u)].wait_recv()
            start(("fx", st, u))
            if st == 1:
                start(("y", 3, u))
            copies[("y", st, u)].wait_recv()
            start(("fy", st, u))
            if st == 1:
                start(("x", 3, u))
        project(st, 0)
        for u in range(NSUB):
            copies[("fx", st, u)].wait_recv()
            copies[("fy", st, u)].wait_recv()
        project(st, tok)
        attend(2 * tok, 0, last=st == 3)

    oc = pltpu.make_async_remote_copy(
        src_ref=osend, dst_ref=orecv, send_sem=osem.at[0], recv_sem=osem.at[1],
        device_id=mate, device_id_type=MESH)
    oc.start()
    loads[4].wait()
    loads[5].wait()
    y = _nn(omine[...], wo[0])
    oc.wait_recv()
    y_ref[...] = (y + _nn(orecv[...], wo[1])).astype(BF16)
    oc.wait_send()
    for key in started:
        copies[key].wait_send()


def solution(mesh):
    def body(x, w_qkv, w_o):
        tok, width = x.shape[1], x.shape[2]
        heads_all, hd = w_o.shape[0], w_o.shape[1]
        heads = heads_all // 2
        cols = heads * hd
        ncopy = 1 + 3 * 4 * NSUB
        y = pl.pallas_call(
            lambda *r: _kernel((tok, width, heads, hd), *r),
            out_shape=jax.ShapeDtypeStruct((tok, width), BF16),
            in_specs=[pl.BlockSpec(memory_space=pl.ANY)] * 3,
            out_specs=pl.BlockSpec(memory_space=pltpu.VMEM),
            scratch_shapes=[
                pltpu.VMEM((4, 2 * tok, width), BF16),
                pltpu.VMEM((width, cols), BF16),
                pltpu.VMEM((width, cols), BF16),
                pltpu.VMEM((width, cols), BF16),
                pltpu.VMEM((cols, width), BF16),
                pltpu.VMEM((2, cols, width), BF16),
                pltpu.VMEM((2 * tok, cols), BF16),
                pltpu.VMEM((cols, 2 * tok), BF16),
                pltpu.VMEM((heads, 2 * hd, 2 * tok), BF16),
                pltpu.VMEM((heads, 1, 2 * tok), F32),
                pltpu.VMEM((heads, 1, 2 * tok), F32),
                pltpu.VMEM((heads, hd, 2 * tok), F32),
                pltpu.VMEM((tok, cols), BF16),
                pltpu.VMEM((tok, cols), BF16),
                pltpu.VMEM((tok, cols), BF16),
                pltpu.VMEM((2 * tok, 2 * tok), F32),
                pltpu.VMEM((2 * tok, 2 * tok), F32),
                pltpu.VMEM((1, 2 * tok), F32),
                pltpu.VMEM((1, 2 * tok), F32),
                pltpu.SemaphoreType.DMA((6,)),
                pltpu.SemaphoreType.DMA((ncopy,)),
                pltpu.SemaphoreType.DMA((ncopy,)),
                pltpu.SemaphoreType.DMA((2,)),
            ],
            compiler_params=pltpu.CompilerParams(
                collective_id=0, has_side_effects=True, vmem_limit_bytes=60 * 1024 * 1024),
            name="dit_attention",
        )(x[0], w_qkv, w_o.reshape(heads_all * hd, width))
        return y[None]

    return jax.shard_map(
        body, mesh=mesh,
        in_specs=(P("dp", ("cx", "cy"), None), P(None, None), P(None, None, None)),
        out_specs=P("dp", ("cx", "cy"), None), check_vma=False)
```

```python
import math

import jax
import jax.numpy as jnp
from jax import lax
from jax.experimental import pallas as pl
from jax.experimental.pallas import tpu as pltpu
from jax.sharding import PartitionSpec as P

MESH = pl.DeviceIdType.MESH
BF16 = jnp.bfloat16
F32 = jnp.float32
UNROLL = 6
AHEAD = 3


def _nt(a, b):
    return lax.dot_general(a, b, (((1,), (1,)), ((), ())), preferred_element_type=F32)


def _tn(a, b):
    return lax.dot_general(a, b, (((0,), (0,)), ((), ())), preferred_element_type=F32)


def _nn(a, b):
    return lax.dot_general(a, b, (((1,), (0,)), ((), ())), preferred_element_type=F32)


def _kernel(dims, x_hbm, wqkv_hbm, o_ref,
            xs, wq, wk, wv, wvt, ks, vts, qz, ms, ls, acc, osend,
            sb0, sb1, sb2, mb0, mb1, mb2,
            wsem, ssem, rsem, osem):
    tok, width, heads, hd = dims
    cols = heads * hd
    scale = (hd ** -0.5) * math.log2(math.e)

    dp, cx, cy = lax.axis_index("dp"), lax.axis_index("cx"), lax.axis_index("cy")
    core = lax.rem(cy, 2)
    mate = (dp, cx, cy + 1 - 2 * core)
    xn = (dp, cx, lax.rem(cy + 2, 4))
    yn = (dp, 1 - cx, cy)

    def wcopy(i, src, dst):
        return pltpu.make_async_copy(src, dst, wsem.at[i])

    g0 = pl.multiple_of(core * cols, cols)
    loads = [
        wcopy(0, x_hbm, xs.at[pl.ds(0, tok), :]),
        wcopy(1, wqkv_hbm.at[:, pl.ds(g0, cols)], wq),
        wcopy(2, wqkv_hbm.at[:, pl.ds(pl.multiple_of(g0 + width, cols), cols)], wk),
        wcopy(3, wqkv_hbm.at[:, pl.ds(pl.multiple_of(g0 + 2 * width, cols), cols)], wv),
    ]
    for ld in loads:
        ld.start()

    barrier = pltpu.get_barrier_semaphore()
    for other in (mate, xn, yn):
        pl.semaphore_signal(barrier, inc=1, device_id=other, device_id_type=MESH)
    pl.semaphore_wait(barrier, 3)

    def copy(sem, row_from, row_to, rows, dev):
        return pltpu.make_async_remote_copy(
            src_ref=xs.at[pl.ds(row_from, rows), :], dst_ref=xs.at[pl.ds(row_to, rows), :],
            send_sem=ssem.at[sem], recv_sem=rsem.at[sem], device_id=dev, device_id_type=MESH)

    part = tok // 4
    x_from = [2 * part, 3 * part, 0, part, 2 * tok + part, 3 * tok + part]
    y_from = [0, part, 2 * part, 3 * part, 2 * tok, 3 * tok]
    from_x = [copy(s, x_from[s], (2 + s) * tok, part, xn) for s in range(6)]
    from_y = [copy(6 + s, y_from[s], (2 + s) * tok + part, part, yn) for s in range(6)]
    from_mate = [copy(12 + s, (2 + s) * tok, (2 + s) * tok + 2 * part, 2 * part, mate) for s in range(6)]
    own = copy(18, 0, tok, tok, mate)

    loads[0].wait()
    own.start()
    for s in range(4):
        from_x[s].start()
        from_y[s].start()

    def arrived(s):
        from_x[s].wait_recv()
        from_y[s].wait_recv()
        from_mate[s].start()
        if s < 2:
            from_x[4 + s].start()
            from_y[4 + s].start()
        if s > 0:
            from_mate[s - 1].wait_recv()

    def project_k(row, r0, rows):
        ks[pl.ds(r0, rows), :] = _nn(xs[pl.ds(row, rows), :], wk[...]).astype(BF16)

    def project_v(row, r0, rows):
        vts[:, pl.ds(r0, rows)] = _nt(wvt[...], xs[pl.ds(row, rows), :]).astype(BF16)

    def project_q(r0):
        rows = xs[pl.ds(r0, tok), :]
        qt = _nn(rows, wq[...]).T.astype(BF16)
        for h in range(heads):
            e = (h % 2) * hd
            qz[h, pl.ds(e, hd), pl.ds(r0, tok)] = qt[h * hd:(h + 1) * hd, :]

    def scores(h, pair, rows, r0, sb, mb):
        kp = ks[pl.ds(r0, rows), pl.ds(pl.multiple_of(pair * 2 * hd, 2 * hd), 2 * hd)]
        s = _nn(kp, qz[h])
        for b in range(2 * tok // 128):
            sb[b, pl.ds(0, rows), :] = s[:, b * 128:(b + 1) * 128]
        mb[...] = jnp.max(s, axis=0, keepdims=True)

    def fold(h, rows, r0, sb, mb, first):
        m = mb[...]
        if not first:
            m = jnp.maximum(ms[h], m)
            alpha = jnp.exp2((ms[h] - m) * scale)
        p = jnp.concatenate([jnp.exp2((sb[b, pl.ds(0, rows), :] - m[:, b * 128:(b + 1) * 128]) * scale) for b in range(2 * tok // 128)], axis=1)
        l = jnp.sum(p, axis=0, keepdims=True)
        o = _nn(vts[pl.ds(pl.multiple_of(h * hd, hd), hd), pl.ds(r0, rows)], p.astype(BF16))
        if not first:
            l = ls[h] * alpha + l
            o = acc[h] * alpha + o
        return m, l, o

    def keep(h, mlo):
        ms[h], ls[h], acc[h] = mlo

    def ocopy(j):
        return pltpu.make_async_remote_copy(
            src_ref=osend.at[:, pl.ds(pl.multiple_of(j * 2 * hd, 2 * hd), 2 * hd)],
            dst_ref=o_ref.at[:, pl.ds(pl.multiple_of(g0 + j * 2 * hd, 2 * hd), 2 * hd)],
            send_sem=osem.at[0, j], recv_sem=osem.at[1, j],
            device_id=mate, device_id_type=MESH)

    def attend(rows, r0, first=False, last=False):
        bufs, maxs = (sb0, sb1, sb2), (mb0, mb1, mb2)
        for d in range(AHEAD):
            scores(d, d // 2, rows, r0, bufs[d], maxs[d])

        def block(j, carry):
            even = None
            for i in range(UNROLL):
                h, k = j * UNROLL + i, i % AHEAD
                got = fold(h, rows, r0, bufs[k], maxs[k], first)
                if not last:
                    keep(h, got)
                n = jnp.minimum(h + AHEAD, heads - 1)
                scores(n, lax.div(n, 2), rows, r0, bufs[k], maxs[k])
                if last and i % 2 == 0:
                    even = got
                elif last:
                    o = jnp.concatenate([even[2] / even[1], got[2] / got[1]], axis=0).T.astype(BF16)
                    p = j * (UNROLL // 2) + i // 2
                    o_ref[:, pl.ds(pl.multiple_of(g0 + p * 2 * hd, 2 * hd), 2 * hd)] = o[:tok]
                    osend[:, pl.ds(pl.multiple_of(p * 2 * hd, 2 * hd), 2 * hd)] = o[tok:]
                    ocopy(p).start()
            return carry

        lax.fori_loop(0, heads // UNROLL, block, 0)

    for h in range(heads):
        e = ((h + 1) % 2) * hd
        qz[h, pl.ds(e, hd), :] = jnp.zeros((hd, 2 * tok), BF16)
    def project(row, r0, rows):
        project_k(row, r0, rows)
        project_v(row, r0, rows)

    loads[1].wait()
    project_q(0)
    loads[2].wait()
    loads[3].wait()
    wvt[...] = wv[...].T
    project(0, 0, tok)
    own.wait_recv()
    project_q(tok)
    project(tok, tok, tok)
    attend(2 * tok, 0, first=True)
    row, keys = 2 * tok, 0
    for s in range(6):
        arrived(s)
        rows = tok if s else tok // 2
        project(row, keys, rows)
        row, keys = row + rows, keys + rows
        if s in (1, 3, 4):
            attend(keys, 0)
            keys = 0
    from_mate[5].wait_recv()
    project(row, keys, tok // 2)
    attend(keys + tok // 2, 0, last=True)

    for j in range(heads // 2):
        ocopy(j).wait_recv()
        ocopy(j).wait_send()
    for c in (own, *from_x, *from_y, *from_mate):
        c.wait_send()


def solution(mesh):
    def body(x, w_qkv, w_o):
        tok, width = x.shape[1], x.shape[2]
        heads_all, hd = w_o.shape[0], w_o.shape[1]
        heads = heads_all // 2
        cols = heads * hd
        ncopy = 19
        o = pl.pallas_call(
            lambda *r: _kernel((tok, width, heads, hd), *r),
            out_shape=pltpu.VMEM((tok, width), BF16),
            in_specs=[pl.BlockSpec(memory_space=pltpu.HBM)] * 2,
            out_specs=pl.BlockSpec(memory_space=pltpu.VMEM),
            scratch_shapes=[
                pltpu.VMEM((8 * tok, width), BF16),
                pltpu.VMEM((width, cols), BF16),
                pltpu.VMEM((width, cols), BF16),
                pltpu.VMEM((width, cols), BF16),
                pltpu.VMEM((cols, width), BF16),
                pltpu.VMEM((2 * tok, cols), BF16),
                pltpu.VMEM((cols, 2 * tok), BF16),
                pltpu.VMEM((heads, 2 * hd, 2 * tok), BF16),
                pltpu.VMEM((heads, 1, 2 * tok), F32),
                pltpu.VMEM((heads, 1, 2 * tok), F32),
                pltpu.VMEM((heads, hd, 2 * tok), F32),
                pltpu.VMEM((tok, cols), BF16),
                pltpu.VMEM((2 * tok // 128, 2 * tok, 128), F32),
                pltpu.VMEM((2 * tok // 128, 2 * tok, 128), F32),
                pltpu.VMEM((2 * tok // 128, 2 * tok, 128), F32),
                pltpu.VMEM((1, 2 * tok), F32),
                pltpu.VMEM((1, 2 * tok), F32),
                pltpu.VMEM((1, 2 * tok), F32),
                pltpu.SemaphoreType.DMA((4,)),
                pltpu.SemaphoreType.DMA((ncopy,)),
                pltpu.SemaphoreType.DMA((ncopy,)),
                pltpu.SemaphoreType.DMA((2, heads // 2)),
            ],
            compiler_params=pltpu.CompilerParams(
                collective_id=0, has_side_effects=True, vmem_limit_bytes=48 * 1024 * 1024),
            name="dit_attention",
        )(pltpu.with_memory_space_constraint(x[0], pltpu.HBM), pltpu.with_memory_space_constraint(w_qkv, pltpu.HBM))
        y = _nn(o, w_o.reshape(heads_all * hd, width))
        return y.astype(BF16)[None]

    return jax.shard_map(
        body, mesh=mesh,
        in_specs=(P("dp", ("cx", "cy"), None), P(None, None), P(None, None, None)),
        out_specs=P("dp", ("cx", "cy"), None), check_vma=False)
```

```python
import math

import jax
import jax.numpy as jnp
from jax import lax
from jax.experimental import pallas as pl
from jax.experimental.pallas import tpu as pltpu
from jax.sharding import PartitionSpec as P

MESH = pl.DeviceIdType.MESH
BF16 = jnp.bfloat16
F32 = jnp.float32
UNROLL = 6
AHEAD = 3


def _nt(a, b):
    return lax.dot_general(a, b, (((1,), (1,)), ((), ())), preferred_element_type=F32)


def _tn(a, b):
    return lax.dot_general(a, b, (((0,), (0,)), ((), ())), preferred_element_type=F32)


def _nn(a, b):
    return lax.dot_general(a, b, (((1,), (0,)), ((), ())), preferred_element_type=F32)


def _kernel(dims, x_hbm, wqkv_hbm, o_ref,
            xs, w, ks, vts, qz, ms, ls, acc, osend,
            sb0, sb1, sb2, mb0, mb1, mb2,
            wsem, ssem, rsem, osem):
    tok, width, heads, hd = dims
    cols = heads * hd
    scale = (hd ** -0.5) * math.log2(math.e)

    dp, cx, cy = lax.axis_index("dp"), lax.axis_index("cx"), lax.axis_index("cy")
    core = lax.rem(cy, 2)
    mate = (dp, cx, cy + 1 - 2 * core)
    xn = (dp, cx, lax.rem(cy + 2, 4))
    yn = (dp, 1 - cx, cy)

    def wcopy(i, src, dst):
        return pltpu.make_async_copy(src, dst, wsem.at[i])

    g0 = pl.multiple_of(core * cols, cols)
    loads = [
        wcopy(0, x_hbm, xs.at[pl.ds(0, tok), :]),
        wcopy(1, wqkv_hbm.at[:, pl.ds(g0, cols)], w.at[:, pl.ds(0, cols)]),
        wcopy(2, wqkv_hbm.at[:, pl.ds(pl.multiple_of(g0 + width, cols), cols)], w.at[:, pl.ds(cols, cols)]),
        wcopy(3, wqkv_hbm.at[:, pl.ds(pl.multiple_of(g0 + 2 * width, cols), cols)], w.at[:, pl.ds(2 * cols, cols)]),
    ]
    for ld in loads:
        ld.start()

    barrier = pltpu.get_barrier_semaphore()
    for other in (mate, xn, yn):
        pl.semaphore_signal(barrier, inc=1, device_id=other, device_id_type=MESH)
    pl.semaphore_wait(barrier, 3)

    def copy(sem, row_from, row_to, rows, dev):
        return pltpu.make_async_remote_copy(
            src_ref=xs.at[pl.ds(row_from, rows), :], dst_ref=xs.at[pl.ds(row_to, rows), :],
            send_sem=ssem.at[sem], recv_sem=rsem.at[sem], device_id=dev, device_id_type=MESH)

    part = tok // 4
    x_from = [2 * part, 3 * part, 0, part, 2 * tok + part, 3 * tok + part]
    y_from = [0, part, 2 * part, 3 * part, 2 * tok, 3 * tok]
    from_x = [copy(s, x_from[s], (2 + s) * tok, part, xn) for s in range(6)]
    from_y = [copy(6 + s, y_from[s], (2 + s) * tok + part, part, yn) for s in range(6)]
    from_mate = [copy(12 + s, (2 + s) * tok, (2 + s) * tok + 2 * part, 2 * part, mate) for s in range(6)]
    own = copy(18, 0, tok, tok, mate)

    loads[0].wait()
    own.start()
    for s in range(4):
        from_x[s].start()
        from_y[s].start()

    def arrived(s):
        from_x[s].wait_recv()
        from_y[s].wait_recv()
        from_mate[s].start()
        if s < 2:
            from_x[4 + s].start()
            from_y[4 + s].start()
        if 0 < s < 5:
            from_mate[s - 1].wait_recv()

    def put_q(q, r0):
        qt = q.T.astype(BF16)
        for h in range(heads):
            e = (h % 2) * hd
            qz[h, pl.ds(e, hd), pl.ds(r0, q.shape[0])] = qt[h * hd:(h + 1) * hd, :]

    def put_kv(kv, r0):
        rows = kv.shape[0]
        ks[pl.ds(r0, rows), :] = kv[:, :cols].astype(BF16)
        vts[:, pl.ds(r0, rows)] = kv[:, cols:].T.astype(BF16)

    def project(row, r0, rows):
        put_kv(_nn(xs[pl.ds(row, rows), :], w[:, pl.ds(cols, 2 * cols)]), r0)

    def scores(h, pair, rows, r0, sb, mb):
        kp = ks[pl.ds(r0, rows), pl.ds(pl.multiple_of(pair * 2 * hd, 2 * hd), 2 * hd)]
        s = _nn(kp, qz[h])
        for b in range(2 * tok // 128):
            sb[b, pl.ds(0, rows), :] = s[:, b * 128:(b + 1) * 128]
        mb[...] = jnp.max(s, axis=0, keepdims=True)

    def fold(h, rows, r0, sb, mb, first):
        m = mb[...]
        if not first:
            m = jnp.maximum(ms[h], m)
            alpha = jnp.exp2((ms[h] - m) * scale)
        p = jnp.concatenate([jnp.exp2((sb[b, pl.ds(0, rows), :] - m[:, b * 128:(b + 1) * 128]) * scale) for b in range(2 * tok // 128)], axis=1)
        l = jnp.sum(p, axis=0, keepdims=True)
        o = _nn(vts[pl.ds(pl.multiple_of(h * hd, hd), hd), pl.ds(r0, rows)], p.astype(BF16))
        if not first:
            l = ls[h] * alpha + l
            o = acc[h] * alpha + o
        return m, l, o

    def keep(h, mlo):
        ms[h], ls[h], acc[h] = mlo

    def ocopy(j):
        return pltpu.make_async_remote_copy(
            src_ref=osend.at[:, pl.ds(pl.multiple_of(j * 2 * hd, 2 * hd), 2 * hd)],
            dst_ref=o_ref.at[:, pl.ds(pl.multiple_of(g0 + j * 2 * hd, 2 * hd), 2 * hd)],
            send_sem=osem.at[0, j], recv_sem=osem.at[1, j],
            device_id=mate, device_id_type=MESH)

    def attend(rows, r0, first=False, last=False):
        bufs, maxs = (sb0, sb1, sb2), (mb0, mb1, mb2)
        for d in range(AHEAD):
            scores(d, d // 2, rows, r0, bufs[d], maxs[d])

        def block(j, carry):
            even = None
            for i in range(UNROLL):
                h, k = j * UNROLL + i, i % AHEAD
                got = fold(h, rows, r0, bufs[k], maxs[k], first)
                if not last:
                    keep(h, got)
                n = jnp.minimum(h + AHEAD, heads - 1)
                scores(n, lax.div(n, 2), rows, r0, bufs[k], maxs[k])
                if last and i % 2 == 0:
                    even = got
                elif last:
                    o = jnp.concatenate([even[2] / even[1], got[2] / got[1]], axis=0).T.astype(BF16)
                    p = j * (UNROLL // 2) + i // 2
                    o_ref[:, pl.ds(pl.multiple_of(g0 + p * 2 * hd, 2 * hd), 2 * hd)] = o[:tok]
                    osend[:, pl.ds(pl.multiple_of(p * 2 * hd, 2 * hd), 2 * hd)] = o[tok:]
                    ocopy(p).start()
            return carry

        lax.fori_loop(0, heads // UNROLL, block, 0)

    for h in range(heads):
        e = ((h + 1) % 2) * hd
        qz[h, pl.ds(e, hd), :] = jnp.zeros((hd, 2 * tok), BF16)
    loads[1].wait()
    put_q(_nn(xs[pl.ds(0, tok), :], w[:, pl.ds(0, cols)]), 0)
    own.wait_recv()
    loads[2].wait()
    loads[3].wait()
    project(0, 0, tok)
    qkv = _nn(xs[pl.ds(tok, tok), :], w[...])
    put_q(qkv[:, :cols], tok)
    put_kv(qkv[:, cols:], tok)
    attend(2 * tok, 0, first=True)

    row, keys = 2 * tok, 0

    def take(rows):
        nonlocal row, keys
        project(row, keys, rows)
        row, keys = row + rows, keys + rows

    half = tok // 2
    for s in range(6):
        arrived(s)
        take(tok if s in (1, 2, 3, 4) else half)
        if s == 4:
            from_mate[4].wait_recv()
            take(half)
        if s == 5:
            from_mate[5].wait_recv()
            take(half)
        if s > 0:
            attend(keys, 0, last=s == 5)
            keys = 0
    for j in range(heads // 2):
        ocopy(j).wait_recv()
        ocopy(j).wait_send()
    for c in (own, *from_x, *from_y, *from_mate):
        c.wait_send()


def solution(mesh):
    def body(x, w_qkv, w_o):
        tok, width = x.shape[1], x.shape[2]
        heads_all, hd = w_o.shape[0], w_o.shape[1]
        heads = heads_all // 2
        cols = heads * hd
        ncopy = 19
        o = pl.pallas_call(
            lambda *r: _kernel((tok, width, heads, hd), *r),
            out_shape=pltpu.VMEM((tok, width), BF16),
            in_specs=[pl.BlockSpec(memory_space=pltpu.HBM)] * 2,
            out_specs=pl.BlockSpec(memory_space=pltpu.VMEM),
            scratch_shapes=[
                pltpu.VMEM((8 * tok, width), BF16),
                pltpu.VMEM((width, 3 * cols), BF16),
                pltpu.VMEM((2 * tok, cols), BF16),
                pltpu.VMEM((cols, 2 * tok), BF16),
                pltpu.VMEM((heads, 2 * hd, 2 * tok), BF16),
                pltpu.VMEM((heads, 1, 2 * tok), F32),
                pltpu.VMEM((heads, 1, 2 * tok), F32),
                pltpu.VMEM((heads, hd, 2 * tok), F32),
                pltpu.VMEM((tok, cols), BF16),
                pltpu.VMEM((2 * tok // 128, 2 * tok, 128), F32),
                pltpu.VMEM((2 * tok // 128, 2 * tok, 128), F32),
                pltpu.VMEM((2 * tok // 128, 2 * tok, 128), F32),
                pltpu.VMEM((1, 2 * tok), F32),
                pltpu.VMEM((1, 2 * tok), F32),
                pltpu.VMEM((1, 2 * tok), F32),
                pltpu.SemaphoreType.DMA((4,)),
                pltpu.SemaphoreType.DMA((ncopy,)),
                pltpu.SemaphoreType.DMA((ncopy,)),
                pltpu.SemaphoreType.DMA((2, heads // 2)),
            ],
            compiler_params=pltpu.CompilerParams(
                collective_id=0, has_side_effects=True, vmem_limit_bytes=48 * 1024 * 1024),
            name="dit_attention",
        )(pltpu.with_memory_space_constraint(x[0], pltpu.HBM), pltpu.with_memory_space_constraint(w_qkv, pltpu.HBM))
        y = _nn(o, w_o.reshape(heads_all * hd, width))
        return y.astype(BF16)[None]

    return jax.shard_map(
        body, mesh=mesh,
        in_specs=(P("dp", ("cx", "cy"), None), P(None, None), P(None, None, None)),
        out_specs=P("dp", ("cx", "cy"), None), check_vma=False)
```

```python
import math

import jax
import jax.numpy as jnp
from jax import lax
from jax.experimental import pallas as pl
from jax.experimental.pallas import tpu as pltpu
from jax.sharding import PartitionSpec as P

MESH = pl.DeviceIdType.MESH
BF16 = jnp.bfloat16
F32 = jnp.float32
UNROLL = 6
AHEAD = 2


def _nt(a, b):
    return lax.dot_general(a, b, (((1,), (1,)), ((), ())), preferred_element_type=F32)


def _tn(a, b):
    return lax.dot_general(a, b, (((0,), (0,)), ((), ())), preferred_element_type=F32)


def _nn(a, b):
    return lax.dot_general(a, b, (((1,), (0,)), ((), ())), preferred_element_type=F32)


def _kernel(dims, x_hbm, wqkv_hbm, wo_hbm, y_ref,
            xs, w, wo, part_ref, o_ref, wo_ref, ks, vts, qz, ms, ls, acc, omine, osend,
            sb0, sb1, sb2, mb0, mb1, mb2,
            wsem, ssem, rsem, osem):
    tok, width, heads, hd = dims
    cols = heads * hd
    scale = (hd ** -0.5) * math.log2(math.e)

    dp, cx, cy = lax.axis_index("dp"), lax.axis_index("cx"), lax.axis_index("cy")
    core = lax.rem(cy, 2)
    one = 1 + lax.div(core, 2)
    mate = (dp, cx, cy + 1 - 2 * core)
    xn = (dp, cx, lax.rem(cy + 2, 4))
    yn = (dp, 1 - cx, cy)

    def wcopy(i, src, dst):
        return pltpu.make_async_copy(src, dst, wsem.at[i])

    g0 = pl.multiple_of(core * cols, cols)
    loads = [
        wcopy(0, x_hbm, xs.at[pl.ds(0, tok), :]),
        wcopy(1, wqkv_hbm.at[:, pl.ds(g0, cols)], w.at[:, pl.ds(0, cols)]),
        wcopy(2, wqkv_hbm.at[:, pl.ds(pl.multiple_of(g0 + width, cols), cols)], w.at[:, pl.ds(cols, cols)]),
        wcopy(3, wqkv_hbm.at[:, pl.ds(pl.multiple_of(g0 + 2 * width, cols), cols)], w.at[:, pl.ds(2 * cols, cols)]),
    ]
    for ld in loads:
        ld.start()
    g1 = pl.multiple_of((1 - core) * cols, cols)
    wo_loads = [wcopy(4, wo_hbm.at[pl.ds(g0, cols), :], wo), wcopy(5, wo_hbm.at[pl.ds(g1, cols), :], wo_ref)]

    barrier = pltpu.get_barrier_semaphore()
    for other in (mate, xn, yn):
        pl.semaphore_signal(barrier, inc=1, device_id=other, device_id_type=MESH)
    pl.semaphore_wait(barrier, 3)

    def copy(sem, row_from, row_to, rows, dev):
        return pltpu.make_async_remote_copy(
            src_ref=xs.at[pl.ds(row_from, rows), :], dst_ref=xs.at[pl.ds(row_to, rows), :],
            send_sem=ssem.at[sem], recv_sem=rsem.at[sem], device_id=dev, device_id_type=MESH)

    part = tok // 4
    x_from = [2 * part, 3 * part, 0, part, 2 * tok + part, 3 * tok + part]
    y_from = [0, part, 2 * part, 3 * part, 2 * tok, 3 * tok]
    from_x = [copy(s, x_from[s], (2 + s) * tok, part, xn) for s in range(6)]
    from_y = [copy(6 + s, y_from[s], (2 + s) * tok + part, part, yn) for s in range(6)]
    from_mate = [copy(12 + s, (2 + s) * tok, (2 + s) * tok + 2 * part, 2 * part, mate) for s in range(6)]
    own = copy(18, 0, tok, tok, mate)

    loads[0].wait()
    own.start()
    for s in range(4):
        from_x[s].start()
        from_y[s].start()

    def arrived(s):
        from_x[s].wait_recv()
        from_y[s].wait_recv()
        from_mate[s].start()
        if s < 2:
            from_x[4 + s].start()
            from_y[4 + s].start()
        if s > 0:
            from_mate[s - 1].wait_recv()

    def put_q(q, r0):
        qt = q.T.astype(BF16)
        for h in range(heads):
            e = (h % 2) * hd
            qz[h, pl.ds(e, hd), pl.ds(r0, q.shape[0])] = qt[h * hd:(h + 1) * hd, :]

    def put_kv(kv, r0):
        rows = kv.shape[0]
        ks[pl.ds(r0, rows), :] = kv[:, :cols].astype(BF16)
        vts[:, pl.ds(r0, rows)] = kv[:, cols:].T.astype(BF16)

    def project(row, r0, rows):
        put_kv(_nn(xs[pl.ds(row, rows), :], w[:, pl.ds(cols, 2 * cols)]), r0)

    def scores(h, pair, rows, r0, sb, mb):
        kp = ks[pl.ds(r0, rows), pl.ds(pl.multiple_of(pair * 2 * hd, 2 * hd), 2 * hd)]
        s = _nn(kp, qz[h])
        for b in range(2 * tok // 128):
            sb[b, pl.ds(0, rows), :] = s[:, b * 128:(b + 1) * 128]
        mb[...] = jnp.max(s, axis=0, keepdims=True)

    def fold(h, rows, r0, sb, mb, first):
        m = mb[...]
        if not first:
            m = jnp.maximum(ms[h], m)
            alpha = jnp.exp2((ms[h] - m) * scale)
        p = jnp.concatenate([jnp.exp2((sb[b, pl.ds(0, rows), :] - m[:, b * 128:(b + 1) * 128]) * scale) for b in range(2 * tok // 128)], axis=1)
        l = jnp.sum(p, axis=0, keepdims=True)
        o = _nn(vts[pl.ds(pl.multiple_of(h * hd, hd), hd), pl.ds(r0, rows)], p.astype(BF16))
        if not first:
            l = ls[h] * alpha + l
            o = acc[h] * alpha + o
        return m, l, o

    def keep(h, mlo):
        ms[h], ls[h], acc[h] = mlo

    def ocopy(j):
        return pltpu.make_async_remote_copy(
            src_ref=osend.at[:, pl.ds(pl.multiple_of(j * 2 * hd, 2 * hd), 2 * hd)],
            dst_ref=o_ref.at[:, pl.ds(pl.multiple_of(j * 2 * hd, 2 * hd), 2 * hd)],
            send_sem=osem.at[0, j], recv_sem=osem.at[1, j],
            device_id=mate, device_id_type=MESH)

    def attend(rows, r0, first=False, last=False):
        bufs, maxs = (sb0, sb1, sb2), (mb0, mb1, mb2)
        for d in range(AHEAD):
            scores(d, d // 2, rows, r0, bufs[d], maxs[d])

        def block(j):
            even = None
            for i in range(UNROLL):
                h = j * UNROLL + i
                k, n = h % 3, (h + AHEAD) % 3
                if h + AHEAD < heads:
                    scores(h + AHEAD, (h + AHEAD) // 2, rows, r0, bufs[n], maxs[n])
                got = fold(h, rows, r0, bufs[k], maxs[k], first)
                if not last:
                    keep(h, got)
                if last and i % 2 == 0:
                    even = got
                elif last:
                    o = jnp.concatenate([even[2] * (1.0 / even[1]), got[2] * (1.0 / got[1])], axis=0).T.astype(BF16)
                    p = h // 2
                    omine[:, pl.ds(p * 2 * hd, 2 * hd)] = o[:tok]
                    osend[:, pl.ds(p * 2 * hd, 2 * hd)] = o[tok:]
                    ocopy(p).start()

        for j in range(heads // UNROLL):
            def body(_, carry, j=j):
                block(j)
                return carry
            lax.fori_loop(0, one, body, 0)

    for h in range(heads):
        e = ((h + 1) % 2) * hd
        qz[h, pl.ds(e, hd), :] = jnp.zeros((hd, 2 * tok), BF16)
    loads[1].wait()
    put_q(_nn(xs[pl.ds(0, tok), :], w[:, pl.ds(0, cols)]), 0)
    own.wait_recv()
    loads[2].wait()
    loads[3].wait()
    project(0, 0, tok)
    qkv = _nn(xs[pl.ds(tok, tok), :], w[...])
    put_q(qkv[:, :cols], tok)
    put_kv(qkv[:, cols:], tok)
    attend(2 * tok, 0, first=True)

    for ld in wo_loads:
        ld.start()
    row, keys = 2 * tok, 0

    def take(rows):
        nonlocal row, keys
        project(row, keys, rows)
        row, keys = row + rows, keys + rows

    for s in range(6):
        arrived(s)
        take(tok if s else tok // 2)
        if 0 < s < 5:
            attend(keys, 0)
            keys = 0
    for c in (own, *from_x, *from_y, *from_mate[:5]):
        c.wait_send()
    from_mate[5].wait_recv()
    take(tok // 2)
    attend(keys, 0, last=True)
    for ld in wo_loads:
        ld.wait()
    early, late = pl.ds(0, cols // 2), pl.ds(cols // 2, cols // 2)
    for j in range(heads // 4):
        ocopy(j).wait_recv()
    part_ref[...] = _nn(omine[...], wo[...]) + _nn(o_ref[:, early], wo_ref[early, :])
    for j in range(heads // 4, heads // 2):
        ocopy(j).wait_recv()
    y_ref[...] = (part_ref[...] + _nn(o_ref[:, late], wo_ref[late, :])).astype(BF16)
    for j in range(heads // 2):
        ocopy(j).wait_send()
    from_mate[5].wait_send()


def _finish(part_ref, o_ref, wo_ref, y_hbm, buf, sem):
    n, _, block = buf.shape
    outs = []
    for i in range(n):
        at = pl.ds(i * block, block)
        buf[i] = (part_ref[:, at] + _nn(o_ref[...], wo_ref[:, at])).astype(BF16)
        outs.append(pltpu.make_async_copy(buf.at[i], y_hbm.at[:, at], sem.at[i]))
        outs[-1].start()
    for out in outs:
        out.wait()


def solution(mesh):
    def body(x, w_qkv, w_o):
        tok, width = x.shape[1], x.shape[2]
        heads_all, hd = w_o.shape[0], w_o.shape[1]
        heads = heads_all // 2
        cols = heads * hd
        ncopy = 19
        hbm = lambda a: pltpu.with_memory_space_constraint(a, pltpu.HBM)
        y = pl.pallas_call(
            lambda *r: _kernel((tok, width, heads, hd), *r),
            out_shape=pltpu.VMEM((tok, width), BF16),
            in_specs=[pl.BlockSpec(memory_space=pltpu.HBM)] * 3,
            out_specs=pl.BlockSpec(memory_space=pltpu.VMEM),
            scratch_shapes=[
                pltpu.VMEM((8 * tok, width), BF16),
                pltpu.VMEM((width, 3 * cols), BF16),
                pltpu.VMEM((cols, width), BF16),
                pltpu.VMEM((tok, width), F32),
                pltpu.VMEM((tok, cols), BF16),
                pltpu.VMEM((cols, width), BF16),
                pltpu.VMEM((2 * tok, cols), BF16),
                pltpu.VMEM((cols, 2 * tok), BF16),
                pltpu.VMEM((heads, 2 * hd, 2 * tok), BF16),
                pltpu.VMEM((heads, 1, 2 * tok), F32),
                pltpu.VMEM((heads, 1, 2 * tok), F32),
                pltpu.VMEM((heads, hd, 2 * tok), F32),
                pltpu.VMEM((tok, cols), BF16),
                pltpu.VMEM((tok, cols), BF16),
                pltpu.VMEM((2 * tok // 128, 2 * tok, 128), F32),
                pltpu.VMEM((2 * tok // 128, 2 * tok, 128), F32),
                pltpu.VMEM((2 * tok // 128, 2 * tok, 128), F32),
                pltpu.VMEM((1, 2 * tok), F32),
                pltpu.VMEM((1, 2 * tok), F32),
                pltpu.VMEM((1, 2 * tok), F32),
                pltpu.SemaphoreType.DMA((6,)),
                pltpu.SemaphoreType.DMA((ncopy,)),
                pltpu.SemaphoreType.DMA((ncopy,)),
                pltpu.SemaphoreType.DMA((2, heads // 2)),
            ],
            compiler_params=pltpu.CompilerParams(
                collective_id=0, has_side_effects=True, vmem_limit_bytes=48 * 1024 * 1024),
            name="dit_attention",
        )(hbm(x[0]), hbm(w_qkv), hbm(w_o.reshape(heads_all * hd, width)))
        return y[None]

    return jax.shard_map(
        body, mesh=mesh,
        in_specs=(P("dp", ("cx", "cy"), None), P(None, None), P(None, None, None)),
        out_specs=P("dp", ("cx", "cy"), None), check_vma=False)
```
